1024 devices in a mesh: gx: 128 (over y, z, core), gy: 8 (over x).
Axes of the slice: x: 8, y: 8, z: 8, core: 2. Of those that a mesh axis runs over, the one named last changes fastest.
Arguments:
- positions: float32 [3, 1024, 64, 128], P(None, 'gx', 'gy'), may hold values from 0 to 12
- charges: float32 [1024, 64, 128], P('gx', 'gy'), may hold values from -4 to 4
- cell_index: int32 [1024, 64, 128], P('gx', 'gy'), may hold values from 0 to 32767, as said below
- task_patch: int32 [128, 8, 32], P('gx', 'gy'), may hold values from 0 to 63
- task_near: int32 [128, 8, 32], P('gx', 'gy'), may hold values from 0 to 8
- task_count: int32 [128, 8], P('gx', 'gy'), may hold values from 1 to 32, as said below
Outputs:
- forces: float32 [3, 1024, 64, 128], P(None, 'gx', 'gy')
- recip_potential: float32 [1024, 64, 128], P('gx', 'gy')
The draws below stay inside these ranges and needn't reach their ends.
Inputs may be any that keep to these rules, and one draw needn't show every extreme that they name: `task_near`: code k names the neighbouring patch at offset (k // 3 - 1, k % 3 - 1) along the two patch dimensions; only slots below task_count are read. `task_patch`: only slots below task_count are read. `task_count`: in each gx row one device has 32 live tasks, and the counts of the devices that share a gx index sum to at most 8 * 16. Each atom lies in the cell that cell_index names: for an atom of local patch row r and column s with coordinates (a, b, e), the cell has z = floor(e * 256 / 12), x = (r * 4 + floor(a * 4 / 12)) // 8, y = (s * 32 + floor(b * 32 / 12)) // 8, and c = (z * 4 + x) * 32 + y.
All inputs are finite; a program needn't handle non-finite values.
Results may differ from the reference program's by a relative error of at most 0.0003.
Values sent between devices are 32-bit elements; how exact they have to be, the bound alone decides.
A program may use at most 32 MiB of HBM per device.

```python
import math
import jax
import jax.numpy as jnp
from jax import lax

PX = 8
PY = 8
APATCH = 128
HOSTCAP = 16
TMAX = 32
XR = 4
YC = 32
GZ = 256
GX = 512
GY = 256
NPX = 1024
NPY = 64
N_GX = 128
N_GY = 8


def draw_task_count(key, part):
    first_key = jax.random.fold_in(key, 11)
    second_key = jax.random.fold_in(key, 23)
    busiest = jax.random.randint(first_key, (N_GX,), 0, N_GY)
    ceiling = (N_GY * HOSTCAP - 2 * HOSTCAP) // (N_GY - 1)
    lighter = jax.random.randint(second_key, (N_GX, N_GY), 1, ceiling + 1)
    column = jnp.arange(N_GY, dtype=jnp.int32)[None, :]
    return jnp.where(column == busiest[:, None], 2 * HOSTCAP, lighter).astype(jnp.int32)


def atom_layout(key):
    shape = (NPX, NPY, APATCH)
    fine_x = jax.random.randint(jax.random.fold_in(key, 101), shape, 0, XR)
    fine_y = jax.random.randint(jax.random.fold_in(key, 103), shape, 0, YC)
    fine_z = jax.random.randint(jax.random.fold_in(key, 107), shape, 0, GZ)
    fraction = jax.random.uniform(jax.random.fold_in(key, 109), (3,) + shape, jnp.float32)
    return (fine_x, fine_y, fine_z, fraction)


def draw_positions(key, part):
    fine_x, fine_y, fine_z, fraction = atom_layout(key)
    coord_x = (fine_x.astype(jnp.float32) + fraction[0]) * (12.0 / XR)
    coord_y = (fine_y.astype(jnp.float32) + fraction[1]) * (12.0 / YC)
    coord_z = (fine_z.astype(jnp.float32) + fraction[2]) * (12.0 / GZ)
    return jnp.stack([coord_x, coord_y, coord_z]).astype(jnp.float32)


def draw_cell_index(key, part):
    fine_x, fine_y, fine_z, fraction = atom_layout(key)
    local_row = (jnp.arange(NPX, dtype=jnp.int32) % PX)[:, None, None]
    local_col = (jnp.arange(NPY, dtype=jnp.int32) % PY)[None, :, None]
    cell_x = (local_row * XR + fine_x) // PX
    cell_y = (local_col * YC + fine_y) // PY
    return (fine_z * (XR * YC) + cell_x * YC + cell_y).astype(jnp.int32)


def place_ends(drawn, key, low, high):
    dims = drawn.shape
    index_at = [jax.random.randint(jax.random.fold_in(key, axis), (), 0, dims[axis]) for axis in range(len(dims))]
    drawn = drawn.at[tuple(index_at)].set(low)
    longest = dims.index(max(dims))
    index_at[longest] = (index_at[longest] + 1) % dims[longest]
    return drawn.at[tuple(index_at)].set(high)


def levels(own_key, extent, cuts, least, high):
    level = 1.0
    for dim, shards_of in cuts:
        steps = jax.random.uniform(jax.random.fold_in(jax.random.fold_in(own_key, 6), dim), (shards_of,), jnp.float32, least / len(cuts), high / len(cuts))
        level = level * jnp.repeat(jnp.exp(steps), extent[dim] // shards_of).reshape((-1,) + (1,) * (len(extent) - 1 - dim))
    return level


def bell_draw(rng, extent, deviation, reach, shards=(), held_as=jnp.bfloat16):
    values = jax.random.normal(rng, extent, jnp.float32) * deviation
    if len(shards) > 0:
        values = levels(rng, extent, shards, -0.22, 0.18) * values
    return jnp.clip(values, min=-reach, max=reach).astype(held_as)


def setup_inputs(seed: int = 0) -> dict:
    arg_keys = jax.random.split(jax.random.key(seed), 7)
    positions = draw_positions(jax.random.fold_in(arg_keys[6], 71), 0)
    charges = bell_draw(arg_keys[1], (NPX, NPY, APATCH), 1.0, 4.0, ((0, 128), (1, 8)), jnp.float32)
    cell_index = draw_cell_index(jax.random.fold_in(arg_keys[6], 71), 0)
    task_patch = place_ends(jax.random.randint(arg_keys[3], (N_GX, N_GY, TMAX), 0, PX * PY), jax.random.fold_in(arg_keys[3], 1), 0, (PX * PY) - 1).astype(jnp.int32)
    task_near = place_ends(jax.random.randint(arg_keys[4], (N_GX, N_GY, TMAX), 0, 9), jax.random.fold_in(arg_keys[4], 1), 0, 8).astype(jnp.int32)
    task_count = draw_task_count(jax.random.fold_in(arg_keys[6], 71), 0)
    return {"positions": positions, "charges": charges, "cell_index": cell_index, "task_patch": task_patch, "task_near": task_near, "task_count": task_count}


SCREEN = 72.0
PATCH_SIDE = 12.0
KERNEL_SCALE = 64.0


def pair_force(first, second):
    delta = first[:3, :, None] - second[:3, None, :]
    dist_sq = jnp.sum(delta * delta, axis=0)
    strength = jnp.exp(-dist_sq / SCREEN) * (dist_sq + 1.0) ** (-1.5)
    weight = first[3][:, None] * second[3][None, :] * strength
    return jnp.sum(weight[None] * delta, axis=2)


def task_inputs(halo, patch, near):
    rows = halo.shape[1] - 2
    cols = halo.shape[2] - 2
    flat = halo.reshape(4, (rows + 2) * (cols + 2), halo.shape[3])
    prow = patch // cols + 1
    pcol = patch % cols + 1
    drow = near // 3 - 1
    dcol = near % 3 - 1
    first = jnp.take(flat, prow * (cols + 2) + pcol, axis=1)
    second = jnp.take(flat, (prow + drow) * (cols + 2) + pcol + dcol, axis=1)
    zeros = jnp.zeros(patch.shape, jnp.float32)
    shift = jnp.stack([drow.astype(jnp.float32) * PATCH_SIDE, dcol.astype(jnp.float32) * PATCH_SIDE, zeros, zeros])
    second = second + shift[:, :, None]
    return jnp.moveaxis(first, 1, 0), jnp.moveaxis(second, 1, 0)


def patch_sum(per_task_force, patch, live, rows, cols):
    indicator_matrix = ((patch[:, None] == jnp.arange(rows * cols, dtype=jnp.int32)[None, :]) & live[:, None]).astype(jnp.float32)
    accumulated_sum = jnp.einsum("ew,esh->swh", indicator_matrix, per_task_force, precision=lax.Precision.HIGHEST)
    return accumulated_sum.reshape(3, rows, cols, per_task_force.shape[2])


def local_forces(halo, patch, near, count):
    rows = halo.shape[1] - 2
    cols = halo.shape[2] - 2
    live = jnp.arange(patch.shape[0], dtype=jnp.int32) < count
    first, second = task_inputs(halo, patch, near)
    per_task_force = jax.vmap(pair_force)(first, second)
    return patch_sum(per_task_force, patch, live, rows, cols)


def cas_table(length):
    steps = jnp.arange(length, dtype=jnp.int32)
    product = (steps[:, None] * steps[None, :]) % length
    angle = (2.0 * math.pi / length) * product.astype(jnp.float32)
    return jnp.cos(angle) + jnp.sin(angle)


def wave_part(freq, length):
    folded = jnp.minimum(freq, length - freq).astype(jnp.float32) / length
    return folded * folded


def influence(depth_freq, row_freq, column_freq, depth_len, row_len, column_len):
    wave_sq = wave_part(depth_freq, depth_len)[:, None, None] + wave_part(row_freq, row_len)[None, :, None] + wave_part(column_freq, column_len)[None, None, :]
    safe = jnp.where(wave_sq > 0, wave_sq, 1.0)
    return jnp.where(wave_sq > 0, 1.0 / (KERNEL_SCALE * safe), 0.0)


def reference(positions, charges, cell_index, task_patch, task_near, task_count):
    atoms = jnp.concatenate([positions, charges[None]], axis=0)
    padded = jnp.pad(atoms, ((0, 0), (1, 1), (1, 1), (0, 0)), mode="wrap")
    devices = N_GX * N_GY
    patches = task_patch.reshape(devices, -1)
    nears = task_near.reshape(devices, -1)
    counts = task_count.reshape(devices)

    def single_device_path(index):
        row = (index // N_GY).astype(jnp.int32)
        col = (index % N_GY).astype(jnp.int32)
        start = (jnp.zeros((), jnp.int32), row * PX, col * PY, jnp.zeros((), jnp.int32))
        block = lax.dynamic_slice(padded, start, (4, PX + 2, PY + 2, APATCH))
        return local_forces(block, patches[index], nears[index], counts[index])

    parts = lax.map(single_device_path, jnp.arange(devices, dtype=jnp.int32))
    forces = parts.reshape(N_GX, N_GY, 3, PX, PY, APATCH).transpose(2, 0, 3, 1, 4, 5).reshape(3, NPX, NPY, APATCH)

    prow = (jnp.arange(NPX, dtype=jnp.int32) // PX)[:, None, None]
    pcol = (jnp.arange(NPY, dtype=jnp.int32) // PY)[None, :, None]
    plane = cell_index // (XR * YC)
    xrow = prow * XR + (cell_index // YC) % XR
    ycol = pcol * YC + cell_index % YC
    grid = jnp.zeros((GZ, GX, GY), jnp.float32).at[plane, xrow, ycol].add(charges)
    cas_x = cas_table(GX)
    cas_y = cas_table(GY)
    cas_z = cas_table(GZ)
    high = lax.Precision.HIGHEST
    spectrum = jnp.einsum("zxy,zn->nxy", grid, cas_z, precision=high)
    spectrum = jnp.einsum("zxy,yk->zxk", spectrum, cas_y, precision=high)
    spectrum = jnp.einsum("zxk,xm->zmk", spectrum, cas_x, precision=high)
    kernel = influence(jnp.arange(GZ, dtype=jnp.int32), jnp.arange(GX, dtype=jnp.int32), jnp.arange(GY, dtype=jnp.int32), GZ, GX, GY)
    scaled = spectrum * kernel
    field = jnp.einsum("zmk,mx->zxk", scaled, cas_x, precision=high)
    field = jnp.einsum("zxk,ky->zxy", field, cas_y, precision=high)
    field = jnp.einsum("nxy,nz->zxy", field, cas_z, precision=high) / (GX * GY * GZ)
    recip_potential = field[plane, xrow, ycol]
    return forces, recip_potential
```

```python
import functools

import jax
import jax.numpy as jnp
import numpy as np
from jax import lax
from jax.experimental import pallas as pl
from jax.experimental.pallas import tpu as pltpu
from jax.sharding import PartitionSpec as P

MESH_ID = pl.DeviceIdType.MESH
F32 = jnp.float32
BF16 = jnp.bfloat16

NX = 128
NY = 8
GX = 512
GY = 256
GZ = 256
TASKS = 32
PATCH_SIDE = 12.0
EXP_SCALE = -1.0 / 72.0


def cas_split(length, rows=None):
    steps = np.arange(length, dtype=np.int64)
    angle = (2.0 * np.pi / length) * ((steps[:, None] * steps[None, :]) % length)
    table = np.cos(angle) + np.sin(angle)
    if rows is not None:
        table = table[:, rows]
    high = table.astype(np.float32).astype(BF16)
    low = (table - high.astype(np.float64)).astype(np.float32).astype(BF16)
    return np.stack([high, low])


def split(value):
    high = value.astype(BF16)
    low = (value - high.astype(F32)).astype(BF16)
    return high, low


def mxu(a, b, dims=((1,), (0,))):
    return lax.dot_general(a, b, (dims, ((), ())), preferred_element_type=F32)


def left_table(table, value):
    high, low = split(value)
    both = mxu(table[0], jnp.concatenate([high, low], axis=1))
    return both[:, :128] + both[:, 128:] + mxu(table[1], high)


def right_table(value, table):
    high, low = split(value)
    m = value.shape[0]
    both = mxu(jnp.concatenate([high, low], axis=0), table[0])
    return both[:m] + both[m:] + mxu(high, table[1])


def lane_block(shape):
    return lax.broadcasted_iota(jnp.int32, shape, 1) // 32


def pick(blocks, lanes):
    out = blocks[3]
    for b in (2, 1, 0):
        out = jnp.where(lanes == b, blocks[b], out)
    return out


def turn(value, blocks):
    blocks = blocks % 4
    return value if blocks == 0 else pltpu.roll(value, 32 * blocks, 1)


def kernel(
    patch_s,
    near_s,
    count_s,
    patch_ref,
    pos_hbm,
    chg_hbm,
    cell_hbm,
    casz_hbm,
    casy_hbm,
    casx_hbm,
    casxt_hbm,
    forces_hbm,
    recip_hbm,
    pos_ref,
    chg_ref,
    cell_ref,
    forces_ref,
    recip_ref,
    casz,
    casy,
    casx,
    casxt,
    halo,
    onehot,
    grid_t,
    influence,
    second,
    task_force,
    send_a,
    recv_a,
    send_b,
    recv_b,
    send_c,
    recv_c,
    send_d,
    recv_d,
    load_sem,
    store_sem,
    halo_send,
    halo_recv,
    ex_send,
    ex_recv,
):
    gx = lax.axis_index("gx")
    gy = lax.axis_index("gy")
    up = lax.rem(gx + 1, NX)
    down = lax.rem(gx + NX - 1, NX)
    right = lax.rem(gy + 1, NY)
    left = lax.rem(gy + NY - 1, NY)
    chip_y, chip_z, core = gx // 16, (gx // 2) % 8, gx % 2

    def column_peer(k):
        dc, dz, dy = k % 2, (k // 2) % 8, k // 16
        return (
            lax.rem(chip_y + dy, 8) * 16 + lax.rem(chip_z + dz, 8) * 2 + lax.rem(core + dc, 2)
        )

    loads = [
        pltpu.make_async_copy(src, dst, load_sem.at[i])
        for i, (src, dst) in enumerate(
            (
                (cell_hbm, cell_ref),
                (chg_hbm, chg_ref),
                (pos_hbm, pos_ref),
                (casz_hbm, casz),
                (casy_hbm, casy),
                (casx_hbm, casx),
                (casxt_hbm, casxt),
            )
        )
    ]
    for load in loads:
        load.start()
    tables = loads[3:]

    barrier = pltpu.get_barrier_semaphore()
    for d in range(1, NY):
        pl.semaphore_signal(
            barrier, 1, device_id={"gx": gx, "gy": lax.rem(gy + d, NY)}, device_id_type=MESH_ID
        )
    for px in (up, down):
        for py in (left, right):
            pl.semaphore_signal(barrier, 1, device_id={"gx": px, "gy": py}, device_id_type=MESH_ID)

    def greet(k, carry):
        pl.semaphore_signal(
            barrier, 1, device_id={"gx": column_peer(k), "gy": gy}, device_id_type=MESH_ID
        )
        return carry

    lax.fori_loop(1, NX, greet, 0)

    for load in loads[:3]:
        load.wait()

    for r in range(8):
        for c in range(3):
            halo[r + 1, 1:9, c, :] = pos_ref[c, r]
        halo[r + 1, 1:9, 3, :] = chg_ref[r]

    z_row = lax.broadcasted_iota(jnp.int32, (GZ, 256), 0)
    eight = lax.broadcasted_iota(jnp.int32, (8, 256), 0)

    def deposit(x, carry):
        for s in range(8):
            cells = jnp.concatenate(
                [cell_ref[2 * x, s : s + 1, :], cell_ref[2 * x + 1, s : s + 1, :]], axis=1
            )
            charge = jnp.concatenate(
                [chg_ref[2 * x, s : s + 1, :], chg_ref[2 * x + 1, s : s + 1, :]], axis=1
            )
            hot = jnp.where(z_row == cells // 128, 1.0, 0.0).astype(BF16)
            onehot[x * 8 + s] = hot
            high = charge.astype(BF16).astype(F32)
            rows = jnp.where(eight < 4, high, charge - high)
            rows = jnp.where(eight % 4 == cells % 4, rows, 0.0).astype(BF16)
            part = mxu(rows, hot, ((1,), (1,)))
            grid_t[x, s] = part[0:4] + part[4:8]
        return carry

    lax.fori_loop(0, 4, deposit, 0)

    kx = lax.broadcasted_iota(jnp.int32, (GX, 128), 0)
    lane = lax.broadcasted_iota(jnp.int32, (GX, 128), 1)
    kz = gy * 32 + lane % 32
    ky = gx * 2 + (lane // 32) % 2

    def wave(freq, length):
        part = jnp.minimum(freq, length - freq).astype(F32) * (1.0 / length)
        return part * part

    wave_sq = wave(kz, GZ) + wave(kx, GX) + wave(ky, GY)
    influence[...] = jnp.where(
        wave_sq > 0, 1.0 / (64.0 * jnp.where(wave_sq > 0, wave_sq, 1.0)), 0.0
    )

    tables[0].wait()
    ztrans = right_table(grid_t[...].reshape(128, GZ), casz)
    quarter = lane_block((32, 128))
    for h in range(2):
        parts = [ztrans[32 * x : 32 * x + 32, 128 * h : 128 * h + 128] for x in range(4)]
        for m in range(4):
            send_a[4 * h + m] = pick([turn(parts[x], x - m) for x in range(4)], quarter)

    pl.semaphore_wait(barrier, NY - 1 + 4 + NX - 1)

    def row_exchange(src, dst, which):
        for d in (4, 3, 5, 2, 6, 1, 7):
            peer = lax.rem(gy + d, NY)
            pltpu.make_async_remote_copy(
                src.at[peer],
                dst.at[gy],
                ex_send.at[which],
                ex_recv.at[which],
                device_id={"gx": gx, "gy": peer},
                device_id_type=MESH_ID,
            ).start()
        dst[gy] = src[gy]

    def row_wait(src, dst, which):
        pltpu.make_async_remote_copy(
            src.at[pl.ds(0, NY - 1)],
            dst.at[pl.ds(0, NY - 1)],
            ex_send.at[which],
            ex_recv.at[which],
            device_id={"gx": gx, "gy": right},
            device_id_type=MESH_ID,
        ).wait()

    def column_exchange(src, dst, which):
        def send(i, carry):
            peer = column_peer(NX - 1 - i)
            pltpu.make_async_remote_copy(
                src.at[peer],
                dst.at[gx],
                ex_send.at[which],
                ex_recv.at[which],
                device_id={"gx": peer, "gy": gy},
                device_id_type=MESH_ID,
            ).start()
            return carry

        lax.fori_loop(0, NX - 1, send, 0)
        dst[gx] = src[gx]

    def column_wait(src, dst, which):
        pltpu.make_async_remote_copy(
            src.at[pl.ds(0, NX - 1)],
            dst.at[pl.ds(0, NX - 1)],
            ex_send.at[which],
            ex_recv.at[which],
            device_id={"gx": up, "gy": gy},
            device_id_type=MESH_ID,
        ).wait()

    row_exchange(send_a, recv_a, 0)

    halo_copies = []
    for n, (dx, dy) in enumerate(
        ((-1, -1), (-1, 0), (-1, 1), (0, -1), (0, 1), (1, -1), (1, 0), (1, 1))
    ):
        px = (down, gx, up)[dx + 1]
        py = (left, gy, right)[dy + 1]
        src_r = {-1: pl.ds(1, 1), 0: pl.ds(1, 8), 1: pl.ds(8, 1)}[dx]
        dst_r = {-1: pl.ds(9, 1), 0: pl.ds(1, 8), 1: pl.ds(0, 1)}[dx]
        src_c = {-1: pl.ds(1, 1), 0: pl.ds(1, 8), 1: pl.ds(8, 1)}[dy]
        dst_c = {-1: pl.ds(9, 1), 0: pl.ds(1, 8), 1: pl.ds(0, 1)}[dy]
        copy = pltpu.make_async_remote_copy(
            halo.at[src_r, src_c],
            halo.at[dst_r, dst_c],
            halo_send.at[n],
            halo_recv.at[n],
            device_id={"gx": px, "gy": py},
            device_id_type=MESH_ID,
        )
        copy.start()
        halo_copies.append(copy)

    tables[1].wait()
    row_wait(send_a, recv_a, 0)
    ytrans = left_table(casy, recv_a[...].reshape(GY, 128))
    send_b[...] = ytrans.reshape(NX, 2, 128)
    column_exchange(send_b, recv_b, 1)

    for copy in halo_copies:
        copy.wait()

    def task_group(g, carry):
        firsts = []
        for t in range(8):
            patch = patch_s[0, 0, 8 * g + t]
            near = near_s[0, 0, 8 * g + t]
            prow, pcol = patch // 8 + 1, patch % 8 + 1
            drow, dcol = near // 3 - 1, near % 3 - 1
            firsts.append((prow, pcol, drow, dcol))
            second[4 * t : 4 * t + 4, :] = halo[prow + drow, pcol + dcol]
        columns = jnp.transpose(second[...])
        for t in range(8):
            prow, pcol, drow, dcol = firsts[t]
            first = halo[prow, pcol]
            ax = first[0:1] - drow.astype(F32) * PATCH_SIDE
            ay = first[1:2] - dcol.astype(F32) * PATCH_SIDE
            az = first[2:3]
            sums = [jnp.zeros((8, 128), F32) for _ in range(3)]
            for chunk in range(4):
                b = columns[32 * chunk : 32 * chunk + 32]
                delta = [
                    a - b[:, 4 * t + c : 4 * t + c + 1] for c, a in enumerate((ax, ay, az))
                ]
                dist = delta[0] * delta[0] + delta[1] * delta[1] + delta[2] * delta[2]
                inv = lax.rsqrt(dist + 1.0)
                weight = b[:, 4 * t + 3 : 4 * t + 4] * jnp.exp(dist * EXP_SCALE) * (inv * inv * inv)
                for c in range(3):
                    term = weight * delta[c]
                    sums[c] = sums[c] + (
                        (term[0:8] + term[8:16]) + (term[16:24] + term[24:32])
                    )
            for c in range(3):
                total = jnp.sum(sums[c], axis=0, keepdims=True) * first[3:4]
                task_force[c, pl.ds(8 * g + t, 1), :] = total
        return carry

    lax.fori_loop(0, TASKS // 8, task_group, 0)
    slot = lax.broadcasted_iota(jnp.int32, (64, TASKS), 1)
    owner = lax.broadcasted_iota(jnp.int32, (64, TASKS), 0)
    acts = jnp.where((owner == patch_ref[0]) & (slot < count_s[0, 0]), 1.0, 0.0).astype(BF16)
    for c in range(3):
        force = task_force[c]
        high = force.astype(BF16)
        rest = force - high.astype(F32)
        mid = rest.astype(BF16)
        low = (rest - mid.astype(F32)).astype(BF16)
        total = mxu(acts, high) + (mxu(acts, mid) + mxu(acts, low))
        forces_ref[c] = total.reshape(8, 8, 128)
    forces_out = pltpu.make_async_copy(forces_ref, forces_hbm, store_sem.at[0])
    forces_out.start()

    tables[2].wait()
    tables[3].wait()
    column_wait(send_b, recv_b, 1)
    lanes = lane_block((NX, 128))
    low_half = lax.broadcasted_iota(jnp.int32, (NX, 128), 1) < 64
    lines = [recv_b[:, e, :] for e in range(2)]
    turned = [[turn(lines[e], d) for d in range(4)] for e in range(2)]
    packed = []
    for x in range(4):
        value = pick([turned[b % 2][(b - x) % 4] for b in range(4)], lanes)
        high = value.astype(BF16).astype(F32)
        packed.append(jnp.where(low_half, high, value - high).astype(BF16))
    packed = jnp.concatenate(packed, axis=0)
    total = mxu(casx[0], packed) + mxu(casx[1], packed)
    scaled = (total + pltpu.roll(total, 64, 1)) * influence[...]
    high = scaled.astype(BF16).astype(F32)
    half = lax.broadcasted_iota(jnp.int32, (GX, 128), 1) < 64
    packed = jnp.where(half, high, scaled - high).astype(BF16)
    total = mxu(casxt[0], packed) + mxu(casxt[1], packed)
    xback = total + pltpu.roll(total, 64, 1)
    plain = [xback[128 * x : 128 * x + 128] for x in range(4)]
    moved = [turn(p, 1) for p in plain]
    send_c[:, 0, :] = pick([plain[0], moved[1], plain[2], moved[3]], lanes)
    send_c[:, 1, :] = pick([moved[0], plain[1], moved[2], plain[3]], lanes)
    column_exchange(send_c, recv_c, 2)

    column_wait(send_c, recv_c, 2)
    yback = left_table(casy, recv_c[...].reshape(GY, 128))
    send_d[...] = yback.reshape(NY, 32, 128)
    row_exchange(send_d, recv_d, 3)
    row_wait(send_d, recv_d, 3)

    rows = []
    for x in range(4):
        halves = []
        for h in range(2):
            halves.append(
                pick([turn(recv_d[4 * h + m], m - x) for m in range(4)], quarter)
            )
        rows.append(jnp.concatenate(halves, axis=1))
    field = right_table(jnp.concatenate(rows, axis=0), casz) * (1.0 / (GX * GY * GZ))
    grid_t[...] = field.reshape(4, 8, 4, GZ)

    def sample(x, carry):
        for s in range(8):
            cells = jnp.concatenate(
                [cell_ref[2 * x, s : s + 1, :], cell_ref[2 * x + 1, s : s + 1, :]], axis=1
            )
            value = grid_t[x, s]
            high = value.astype(BF16).astype(F32)
            both = jnp.concatenate([high, value - high], axis=0).astype(BF16)
            got = mxu(both, onehot[x * 8 + s])
            got = jnp.sum(jnp.where(eight % 4 == cells % 4, got, 0.0), axis=0, keepdims=True)
            recip_ref[2 * x, s : s + 1, :] = got[:, :128]
            recip_ref[2 * x + 1, s : s + 1, :] = got[:, 128:]
        return carry

    lax.fori_loop(0, 4, sample, 0)
    recip_out = pltpu.make_async_copy(recip_ref, recip_hbm, store_sem.at[1])
    recip_out.start()
    forces_out.wait()
    recip_out.wait()


def body(positions, charges, cell_index, task_patch, task_near, task_count):
    casz = cas_split(GZ)
    casy = cas_split(GY)
    order = (4 * np.arange(NX)[None, :] + np.arange(4)[:, None]).reshape(-1)
    casx = cas_split(GX, order)
    casxt = np.ascontiguousarray(np.swapaxes(casx, 1, 2))
    vmem = pl.BlockSpec(memory_space=pltpu.VMEM)
    smem = pl.BlockSpec(memory_space=pltpu.SMEM)
    hbm = pl.BlockSpec(memory_space=pltpu.HBM)
    return pl.pallas_call(
        kernel,
        out_shape=(
            jax.ShapeDtypeStruct((3, 8, 8, 128), F32),
            jax.ShapeDtypeStruct((8, 8, 128), F32),
        ),
        in_specs=[smem] * 3 + [vmem] + [hbm] * 7,
        out_specs=(hbm, hbm),
        scratch_shapes=[
            pltpu.VMEM((3, 8, 8, 128), F32),
            pltpu.VMEM((8, 8, 128), F32),
            pltpu.VMEM((8, 8, 128), jnp.int32),
            pltpu.VMEM((3, 8, 8, 128), F32),
            pltpu.VMEM((8, 8, 128), F32),
            pltpu.VMEM((2, GZ, GZ), BF16),
            pltpu.VMEM((2, GY, GY), BF16),
            pltpu.VMEM((2, GX, GX), BF16),
            pltpu.VMEM((2, GX, GX), BF16),
            pltpu.VMEM((10, 10, 4, 128), F32),
            pltpu.VMEM((32, GZ, 256), BF16),
            pltpu.VMEM((4, 8, 4, GZ), F32),
            pltpu.VMEM((GX, 128), F32),
            pltpu.VMEM((32, 128), F32),
            pltpu.VMEM((3, TASKS, 128), F32),
            pltpu.VMEM((NY, 32, 128), F32),
            pltpu.VMEM((NY, 32, 128), F32),
            pltpu.VMEM((NX, 2, 128), F32),
            pltpu.VMEM((NX, 2, 128), F32),
            pltpu.VMEM((NX, 2, 128), F32),
            pltpu.VMEM((NX, 2, 128), F32),
            pltpu.VMEM((NY, 32, 128), F32),
            pltpu.VMEM((NY, 32, 128), F32),
            pltpu.SemaphoreType.DMA((7,)),
            pltpu.SemaphoreType.DMA((2,)),
            pltpu.SemaphoreType.DMA((8,)),
            pltpu.SemaphoreType.DMA((8,)),
            pltpu.SemaphoreType.DMA((4,)),
            pltpu.SemaphoreType.DMA((4,)),
        ],
        compiler_params=pltpu.CompilerParams(
            collective_id=0, has_side_effects=True, vmem_limit_bytes=67_043_328
        ),
        name="patch_forces_and_grid",
    )(
        task_patch,
        task_near,
        task_count,
        task_patch,
        positions,
        charges,
        cell_index,
        casz,
        casy,
        casx,
        casxt,
    )


def solution(mesh):
    return jax.shard_map(
        body,
        mesh=mesh,
        in_specs=(
            P(None, "gx", "gy", None),
            P("gx", "gy", None),
            P("gx", "gy", None),
            P("gx", "gy", None),
            P("gx", "gy", None),
            P("gx", "gy"),
        ),
        out_specs=(P(None, "gx", "gy", None), P("gx", "gy", None)),
        check_vma=False,
    )
```

```python
import functools

import jax
import jax.numpy as jnp
import numpy as np
from jax import lax
from jax.experimental import pallas as pl
from jax.experimental.pallas import tpu as pltpu
from jax.sharding import PartitionSpec as P

MESH_ID = pl.DeviceIdType.MESH
F32 = jnp.float32
BF16 = jnp.bfloat16

NX = 128
NY = 8
GX = 512
GY = 256
GZ = 256
TASKS = 32
PATCH_SIDE = 12.0
EXP_SCALE = -1.0 / 72.0


def cas_split(length, rows=None):
    steps = np.arange(length, dtype=np.int64)
    angle = (2.0 * np.pi / length) * ((steps[:, None] * steps[None, :]) % length)
    table = np.cos(angle) + np.sin(angle)
    if rows is not None:
        table = table[:, rows]
    high = table.astype(np.float32).astype(BF16)
    low = (table - high.astype(np.float64)).astype(np.float32).astype(BF16)
    return np.stack([high, low])


def split(value):
    high = value.astype(BF16)
    low = (value - high.astype(F32)).astype(BF16)
    return high, low


def mxu(a, b, dims=((1,), (0,))):
    return lax.dot_general(a, b, (dims, ((), ())), preferred_element_type=F32)


def left_table(table, value):
    high, low = split(value)
    both = mxu(table[0], jnp.concatenate([high, low], axis=1))
    return both[:, :128] + both[:, 128:] + mxu(table[1], high)


def right_table(value, table):
    high, low = split(value)
    m = value.shape[0]
    both = mxu(jnp.concatenate([high, low], axis=0), table[0])
    return both[:m] + both[m:] + mxu(high, table[1])


def lane_block(shape):
    return lax.broadcasted_iota(jnp.int32, shape, 1) // 32


def pick(blocks, lanes):
    out = blocks[3]
    for b in (2, 1, 0):
        out = jnp.where(lanes == b, blocks[b], out)
    return out


def turn(value, blocks):
    blocks = blocks % 4
    return value if blocks == 0 else pltpu.roll(value, 32 * blocks, 1)


def kernel(
    patch_hbm,
    near_hbm,
    count_hbm,
    pos_hbm,
    chg_hbm,
    cell_hbm,
    casz_hbm,
    casy_hbm,
    casx_hbm,
    casxt_hbm,
    forces_ref,
    recip_ref,
    patch_s,
    near_s,
    patch_ref,
    count_ref,
    pos_ref,
    chg_ref,
    cell_ref,
    casz,
    casy,
    casx,
    casxt,
    halo,
    grid_t,
    sampled,
    influence,
    second,
    task_force,
    send_a,
    recv_a,
    send_b,
    recv_b,
    send_c,
    recv_c,
    send_d,
    recv_d,
    load_sem,
    halo_send,
    halo_recv,
    ex_send,
    ex_recv,
):
    gx = lax.axis_index("gx")
    gy = lax.axis_index("gy")
    up = lax.rem(gx + 1, NX)
    down = lax.rem(gx + NX - 1, NX)
    right = lax.rem(gy + 1, NY)
    left = lax.rem(gy + NY - 1, NY)
    chip_y, chip_z, core = gx // 16, (gx // 2) % 8, gx % 2

    across = [
        lax.rem(chip_z + dz, 8) * 2 + lax.rem(core + dc, 2) for dz in range(8) for dc in range(2)
    ]

    def each_column_peer(visit):
        def chip_row(i, carry):
            base = lax.rem(chip_y + 12 - i - i // 4, 8) * 16
            for other in across:
                visit(base + other)
            return carry

        lax.fori_loop(0, 7, chip_row, 0)
        for other in across[1:]:
            visit(chip_y * 16 + other)

    loads = [
        pltpu.make_async_copy(src, dst, load_sem.at[i])
        for i, (src, dst) in enumerate(
            (
                (cell_hbm, cell_ref),
                (chg_hbm, chg_ref),
                (casz_hbm, casz),
                (casy_hbm, casy),
                (casx_hbm, casx),
                (casxt_hbm, casxt),
                (pos_hbm, pos_ref),
                (patch_hbm, patch_s),
                (near_hbm, near_s),
                (patch_hbm, patch_ref),
                (count_hbm, count_ref),
            )
        )
    ]
    for load in loads[:2]:
        load.start()
    tables = loads[2:6]
    task_loads = loads[7:]

    barrier = pltpu.get_barrier_semaphore()
    for d in range(1, NY):
        pl.semaphore_signal(
            barrier, 1, device_id={"gx": gx, "gy": lax.rem(gy + d, NY)}, device_id_type=MESH_ID
        )
    for px in (up, down):
        for py in (left, right):
            pl.semaphore_signal(barrier, 1, device_id={"gx": px, "gy": py}, device_id_type=MESH_ID)

    each_column_peer(
        lambda peer: pl.semaphore_signal(
            barrier, 1, device_id={"gx": peer, "gy": gy}, device_id_type=MESH_ID
        )
    )

    for load in loads[2:]:
        load.start()
    loads[0].wait()
    loads[1].wait()

    eight = lax.broadcasted_iota(jnp.int32, (8, 256), 0)
    z_lane = lax.broadcasted_iota(jnp.int32, (128, GZ), 1)

    def atoms_of(ref, x, s):
        return jnp.concatenate([ref[2 * x, s : s + 1, :], ref[2 * x + 1, s : s + 1, :]], axis=1)

    def deposit(x, carry):
        planes = jnp.concatenate([cell_ref[2 * x], cell_ref[2 * x + 1]], axis=0) // 128
        planes = jnp.transpose(planes)
        for s in range(8):
            cells = atoms_of(cell_ref, x, s)
            charge = atoms_of(chg_ref, x, s)
            hot = jnp.concatenate(
                [
                    jnp.where(z_lane == planes[:, 8 * r + s : 8 * r + s + 1], 1.0, 0.0).astype(BF16)
                    for r in range(2)
                ],
                axis=0,
            )
            high = charge.astype(BF16).astype(F32)
            rows = jnp.where(eight < 4, high, charge - high)
            rows = jnp.where(eight % 4 == cells % 4, rows, 0.0).astype(BF16)
            part = mxu(rows, hot)
            grid_t[x, s] = part[0:4] + part[4:8]
        return carry

    lax.fori_loop(0, 4, deposit, 0, unroll=True)

    tables[0].wait()
    ztrans = right_table(grid_t[...].reshape(128, GZ), casz)
    quarter = lane_block((32, 128))
    for h in range(2):
        parts = [ztrans[32 * x : 32 * x + 32, 128 * h : 128 * h + 128] for x in range(4)]
        for m in range(4):
            send_a[4 * h + m] = pick([turn(parts[x], x - m) for x in range(4)], quarter)

    pl.semaphore_wait(barrier, NY - 1 + 4 + NX - 1)

    def row_exchange(src, dst, which):
        for d in (4, 3, 5, 2, 6, 1, 7):
            peer = lax.rem(gy + d, NY)
            pltpu.make_async_remote_copy(
                src.at[peer],
                dst.at[gy],
                ex_send.at[which],
                ex_recv.at[which],
                device_id={"gx": gx, "gy": peer},
                device_id_type=MESH_ID,
            ).start()
        dst[gy] = src[gy]

    def row_wait(src, dst, which):
        pltpu.make_async_remote_copy(
            src.at[pl.ds(0, NY - 1)],
            dst.at[pl.ds(0, NY - 1)],
            ex_send.at[which],
            ex_recv.at[which],
            device_id={"gx": gx, "gy": right},
            device_id_type=MESH_ID,
        ).wait()

    def column_exchange(src, dst, which):
        each_column_peer(
            lambda peer: pltpu.make_async_remote_copy(
                src.at[peer],
                dst.at[gx],
                ex_send.at[which],
                ex_recv.at[which],
                device_id={"gx": peer, "gy": gy},
                device_id_type=MESH_ID,
            ).start()
        )
        dst[gx] = src[gx]

    def column_wait(src, dst, which):
        pltpu.make_async_remote_copy(
            src.at[pl.ds(0, NX - 1)],
            dst.at[pl.ds(0, NX - 1)],
            ex_send.at[which],
            ex_recv.at[which],
            device_id={"gx": up, "gy": gy},
            device_id_type=MESH_ID,
        ).wait()

    row_exchange(send_a, recv_a, 0)

    kx = lax.broadcasted_iota(jnp.int32, (GX, 128), 0)
    lane = lax.broadcasted_iota(jnp.int32, (GX, 128), 1)
    kz = gy * 32 + lane % 32
    ky = gx * 2 + (lane // 32) % 2

    def wave(freq, length):
        part = jnp.minimum(freq, length - freq).astype(F32) * (1.0 / length)
        return part * part

    wave_sq = wave(kz, GZ) + wave(kx, GX) + wave(ky, GY)
    influence[...] = jnp.where(
        wave_sq > 0, 1.0 / (64.0 * jnp.where(wave_sq > 0, wave_sq, 1.0)), 0.0
    )

    tables[1].wait()
    row_wait(send_a, recv_a, 0)
    ytrans = left_table(casy, recv_a[...].reshape(GY, 128))
    send_b[...] = ytrans.reshape(NX, 2, 128)
    column_exchange(send_b, recv_b, 1)

    loads[6].wait()
    for r in range(8):
        for c in range(3):
            halo[r + 1, 1:9, c, :] = pos_ref[c, r]
        halo[r + 1, 1:9, 3, :] = chg_ref[r]

    halo_copies = []
    for n, (dx, dy) in enumerate(
        ((-1, -1), (-1, 0), (-1, 1), (0, -1), (0, 1), (1, -1), (1, 0), (1, 1))
    ):
        px = (down, gx, up)[dx + 1]
        py = (left, gy, right)[dy + 1]
        src_r = {-1: pl.ds(1, 1), 0: pl.ds(1, 8), 1: pl.ds(8, 1)}[dx]
        dst_r = {-1: pl.ds(9, 1), 0: pl.ds(1, 8), 1: pl.ds(0, 1)}[dx]
        src_c = {-1: pl.ds(1, 1), 0: pl.ds(1, 8), 1: pl.ds(8, 1)}[dy]
        dst_c = {-1: pl.ds(9, 1), 0: pl.ds(1, 8), 1: pl.ds(0, 1)}[dy]
        copy = pltpu.make_async_remote_copy(
            halo.at[src_r, src_c],
            halo.at[dst_r, dst_c],
            halo_send.at[n],
            halo_recv.at[n],
            device_id={"gx": px, "gy": py},
            device_id_type=MESH_ID,
        )
        copy.start()
        halo_copies.append(copy)

    tables[2].wait()
    tables[3].wait()
    column_wait(send_b, recv_b, 1)
    lanes = lane_block((NX, 128))
    low_half = lax.broadcasted_iota(jnp.int32, (NX, 128), 1) < 64
    lines = [recv_b[:, e, :] for e in range(2)]
    turned = [[turn(lines[e], d) for d in range(4)] for e in range(2)]
    packed = []
    for x in range(4):
        value = pick([turned[b % 2][(b - x) % 4] for b in range(4)], lanes)
        high = value.astype(BF16).astype(F32)
        packed.append(jnp.where(low_half, high, value - high).astype(BF16))
    packed = jnp.concatenate(packed, axis=0)
    total = mxu(casx[0], packed) + mxu(casx[1], packed)
    scaled = (total + pltpu.roll(total, 64, 1)) * influence[...]
    high = scaled.astype(BF16).astype(F32)
    half = lax.broadcasted_iota(jnp.int32, (GX, 128), 1) < 64
    packed = jnp.where(half, high, scaled - high).astype(BF16)
    total = mxu(casxt[0], packed) + mxu(casxt[1], packed)
    xback = total + pltpu.roll(total, 64, 1)
    plain = [xback[128 * x : 128 * x + 128] for x in range(4)]
    moved = [turn(p, 1) for p in plain]
    send_c[:, 0, :] = pick([plain[0], moved[1], plain[2], moved[3]], lanes)
    send_c[:, 1, :] = pick([moved[0], plain[1], moved[2], plain[3]], lanes)
    column_exchange(send_c, recv_c, 2)

    for copy in task_loads + halo_copies:
        copy.wait()

    def task_group(g, carry):
        firsts = []
        for t in range(8):
            patch = patch_s[0, 0, 8 * g + t]
            near = near_s[0, 0, 8 * g + t]
            prow, pcol = patch // 8 + 1, patch % 8 + 1
            drow, dcol = near // 3 - 1, near % 3 - 1
            firsts.append((prow, pcol, drow, dcol))
            second[4 * t : 4 * t + 4, :] = halo[prow + drow, pcol + dcol]
        columns = jnp.transpose(second[...])
        for t in range(8):
            prow, pcol, drow, dcol = firsts[t]
            first = halo[prow, pcol]
            ax = first[0:1] - drow.astype(F32) * PATCH_SIDE
            ay = first[1:2] - dcol.astype(F32) * PATCH_SIDE
            az = first[2:3]
            sums = [jnp.zeros((8, 128), F32) for _ in range(3)]
            for chunk in range(4):
                b = columns[32 * chunk : 32 * chunk + 32]
                delta = [
                    a - b[:, 4 * t + c : 4 * t + c + 1] for c, a in enumerate((ax, ay, az))
                ]
                dist = delta[0] * delta[0] + delta[1] * delta[1] + delta[2] * delta[2]
                inv = lax.rsqrt(dist + 1.0)
                weight = b[:, 4 * t + 3 : 4 * t + 4] * jnp.exp(dist * EXP_SCALE) * (inv * inv * inv)
                for c in range(3):
                    term = weight * delta[c]
                    sums[c] = sums[c] + (
                        (term[0:8] + term[8:16]) + (term[16:24] + term[24:32])
                    )
            for c in range(3):
                total = jnp.sum(sums[c], axis=0, keepdims=True) * first[3:4]
                task_force[c, pl.ds(8 * g + t, 1), :] = total
        return carry

    lax.fori_loop(0, TASKS // 8, task_group, 0)
    slot = lax.broadcasted_iota(jnp.int32, (64, TASKS), 1)
    owner = lax.broadcasted_iota(jnp.int32, (64, TASKS), 0)
    acts = jnp.where((owner == patch_ref[0]) & (slot < count_ref[...]), 1.0, 0.0).astype(BF16)
    for c in range(3):
        force = task_force[c]
        high = force.astype(BF16)
        rest = force - high.astype(F32)
        mid = rest.astype(BF16)
        low = (rest - mid.astype(F32)).astype(BF16)
        total = mxu(acts, high) + (mxu(acts, mid) + mxu(acts, low))
        forces_ref[c] = total.reshape(8, 8, 128)

    column_wait(send_c, recv_c, 2)
    yback = left_table(casy, recv_c[...].reshape(GY, 128))
    send_d[...] = yback.reshape(NY, 32, 128)
    row_exchange(send_d, recv_d, 3)
    row_wait(send_d, recv_d, 3)

    rows = []
    for x in range(4):
        halves = []
        for h in range(2):
            halves.append(
                pick([turn(recv_d[4 * h + m], m - x) for m in range(4)], quarter)
            )
        rows.append(jnp.concatenate(halves, axis=1))
    field = right_table(jnp.concatenate(rows, axis=0), casz) * (1.0 / (GX * GY * GZ))
    for h in range(2):
        half_z = field[:, 128 * h : 128 * h + 128].reshape(32, 4, 128)
        sampled[:, 4 * h : 4 * h + 4, :] = half_z

    row_code = lax.broadcasted_iota(jnp.int32, (8, 128), 0)
    for r in range(8):
        for s in range(8):
            cells = jnp.broadcast_to(cell_ref[r, s : s + 1, :], (8, 128))
            planes = cells // 128
            got = jnp.take_along_axis(sampled[(r // 2) * 8 + s], planes % 128, axis=1)
            code = (planes // 128) * 4 + cells % 4
            recip_ref[r, s : s + 1, :] = jnp.sum(
                jnp.where(row_code == code, got, 0.0), axis=0, keepdims=True
            )


def in_hbm(array):
    return pltpu.with_memory_space_constraint(array, pltpu.HBM)


def body(positions, charges, cell_index, task_patch, task_near, task_count):
    casz = cas_split(GZ)
    casy = cas_split(GY)
    order = (4 * np.arange(NX)[None, :] + np.arange(4)[:, None]).reshape(-1)
    casx = cas_split(GX, order)
    casxt = np.ascontiguousarray(np.swapaxes(casx, 1, 2))
    hbm = pl.BlockSpec(memory_space=pltpu.HBM)
    return pl.pallas_call(
        kernel,
        out_shape=(
            pltpu.VMEM((3, 8, 8, 128), F32),
            pltpu.VMEM((8, 8, 128), F32),
        ),
        in_specs=[hbm] * 10,
        out_specs=(pl.BlockSpec(memory_space=pltpu.VMEM),) * 2,
        scratch_shapes=[
            pltpu.SMEM((1, 1, TASKS), jnp.int32),
            pltpu.SMEM((1, 1, TASKS), jnp.int32),
            pltpu.VMEM((1, 1, TASKS), jnp.int32),
            pltpu.VMEM((1, 1), jnp.int32),
            pltpu.VMEM((3, 8, 8, 128), F32),
            pltpu.VMEM((8, 8, 128), F32),
            pltpu.VMEM((8, 8, 128), jnp.int32),
            pltpu.VMEM((2, GZ, GZ), BF16),
            pltpu.VMEM((2, GY, GY), BF16),
            pltpu.VMEM((2, GX, GX), BF16),
            pltpu.VMEM((2, GX, GX), BF16),
            pltpu.VMEM((10, 10, 4, 128), F32),
            pltpu.VMEM((4, 8, 4, GZ), F32),
            pltpu.VMEM((32, 8, 128), F32),
            pltpu.VMEM((GX, 128), F32),
            pltpu.VMEM((32, 128), F32),
            pltpu.VMEM((3, TASKS, 128), F32),
            pltpu.VMEM((NY, 32, 128), F32),
            pltpu.VMEM((NY, 32, 128), F32),
            pltpu.VMEM((NX, 2, 128), F32),
            pltpu.VMEM((NX, 2, 128), F32),
            pltpu.VMEM((NX, 2, 128), F32),
            pltpu.VMEM((NX, 2, 128), F32),
            pltpu.VMEM((NY, 32, 128), F32),
            pltpu.VMEM((NY, 32, 128), F32),
            pltpu.SemaphoreType.DMA((11,)),
            pltpu.SemaphoreType.DMA((8,)),
            pltpu.SemaphoreType.DMA((8,)),
            pltpu.SemaphoreType.DMA((4,)),
            pltpu.SemaphoreType.DMA((4,)),
        ],
        compiler_params=pltpu.CompilerParams(
            collective_id=0, has_side_effects=True, vmem_limit_bytes=60 * 1024 * 1024
        ),
        name="patch_forces_and_grid",
    )(
        in_hbm(task_patch),
        in_hbm(task_near),
        task_count,
        in_hbm(positions),
        in_hbm(charges),
        in_hbm(cell_index),
        in_hbm(jnp.asarray(casz)),
        in_hbm(jnp.asarray(casy)),
        in_hbm(jnp.asarray(casx)),
        in_hbm(jnp.asarray(casxt)),
    )


def solution(mesh):
    return jax.shard_map(
        body,
        mesh=mesh,
        in_specs=(
            P(None, "gx", "gy", None),
            P("gx", "gy", None),
            P("gx", "gy", None),
            P("gx", "gy", None),
            P("gx", "gy", None),
            P("gx", "gy"),
        ),
        out_specs=(P(None, "gx", "gy", None), P("gx", "gy", None)),
        check_vma=False,
    )
```

```python
import functools

import jax
import jax.numpy as jnp
import numpy as np
from jax import lax
from jax.experimental import pallas as pl
from jax.experimental.pallas import tpu as pltpu
from jax.sharding import PartitionSpec as P

MESH_ID = pl.DeviceIdType.MESH
F32 = jnp.float32
BF16 = jnp.bfloat16

NX = 128
NY = 8
GX = 512
GY = 256
GZ = 256
TASKS = 32
PATCH_SIDE = 12.0
EXP_SCALE = -1.0 / 72.0


def cas_split(length, rows=None):
    steps = np.arange(length, dtype=np.int64)
    angle = (2.0 * np.pi / length) * ((steps[:, None] * steps[None, :]) % length)
    table = np.cos(angle) + np.sin(angle)
    if rows is not None:
        table = table[:, rows]
    high = table.astype(np.float32).astype(BF16)
    low = (table - high.astype(np.float64)).astype(np.float32).astype(BF16)
    return np.stack([high, low])


def split(value):
    high = value.astype(BF16)
    low = (value - high.astype(F32)).astype(BF16)
    return high, low


def mxu(a, b, dims=((1,), (0,))):
    return lax.dot_general(a, b, (dims, ((), ())), preferred_element_type=F32)


def left_table(table, value):
    high, low = split(value)
    both = mxu(table[0], jnp.concatenate([high, low], axis=1))
    return both[:, :128] + both[:, 128:] + mxu(table[1], high)


def right_table(value, table):
    high, low = split(value)
    m = value.shape[0]
    both = mxu(jnp.concatenate([high, low], axis=0), table[0])
    return both[:m] + both[m:] + mxu(high, table[1])


def x_transform(table, packed):
    halves = []
    for h in range(2):
        rows = slice(GX // 2 * h, GX // 2 * (h + 1))
        halves.append(mxu(table[0, rows], packed) + mxu(table[1, rows], packed))
    total = jnp.concatenate(halves, axis=0)
    return total + pltpu.roll(total, 64, 1)


def lane_block(shape):
    return lax.broadcasted_iota(jnp.int32, shape, 1) // 32


def pick(blocks, lanes):
    out = blocks[3]
    for b in (2, 1, 0):
        out = jnp.where(lanes == b, blocks[b], out)
    return out


def turn(value, blocks):
    blocks = blocks % 4
    return value if blocks == 0 else pltpu.roll(value, 32 * blocks, 1)


def kernel(
    patch_hbm,
    near_hbm,
    count_hbm,
    pos_hbm,
    chg_hbm,
    cell_hbm,
    casz_hbm,
    casy_hbm,
    casx_hbm,
    casxt_hbm,
    forces_ref,
    recip_ref,
    patch_s,
    near_s,
    patch_ref,
    count_ref,
    pos_ref,
    chg_ref,
    cell_ref,
    casz,
    casy,
    casx,
    casxt,
    halo,
    grid_t,
    sampled,
    influence,
    second,
    task_force,
    send_a,
    recv_a,
    send_b,
    recv_b,
    send_c,
    recv_c,
    send_d,
    recv_d,
    load_sem,
    halo_send,
    halo_recv,
    ex_send,
    ex_recv,
    line_sem,
):
    gx = lax.axis_index("gx")
    gy = lax.axis_index("gy")
    up = lax.rem(gx + 1, NX)
    down = lax.rem(gx + NX - 1, NX)
    right = lax.rem(gy + 1, NY)
    left = lax.rem(gy + NY - 1, NY)
    chip_y, chip_z, core = gx // 16, (gx // 2) % 8, gx % 2

    far_first = (4, 3, 5, 2, 6, 1, 7, 0)
    across = [
        lax.rem(chip_z + dz, 8) * 2 + lax.rem(core + dc, 2) for dz in far_first for dc in (1, 0)
    ]

    def each_column_peer(visit):
        def chip_row(i, carry):
            dy = 4 + (1 - 2 * (i % 2)) * ((i + 1) // 2)
            base = lax.rem(chip_y + dy, 8) * 16
            for other in across:
                visit(base + other)
            return carry

        lax.fori_loop(0, 7, chip_row, 0)
        for other in across[:-1]:
            visit(chip_y * 16 + other)

    loads = [
        pltpu.make_async_copy(src, dst, load_sem.at[i])
        for i, (src, dst) in enumerate(
            (
                (cell_hbm, cell_ref),
                (chg_hbm, chg_ref),
                (casz_hbm, casz),
                (casy_hbm, casy),
                (casx_hbm, casx),
                (casxt_hbm, casxt),
                (pos_hbm, pos_ref),
                (patch_hbm, patch_s),
                (near_hbm, near_s),
                (patch_hbm, patch_ref),
                (count_hbm, count_ref),
            )
        )
    ]
    for load in loads[:2]:
        load.start()
    tables = loads[2:6]
    task_loads = loads[7:]

    barrier = pltpu.get_barrier_semaphore()

    def signal(semaphore, px, py):
        pl.semaphore_signal(semaphore, 1, device_id={"gx": px, "gy": py}, device_id_type=MESH_ID)

    ring_y = [
        lax.rem(chip_y + dy, 8) * 16 + chip_z * 2 + core for dy in far_first[:-1]
    ]
    for d in far_first[:-1]:
        signal(barrier, gx, lax.rem(gy + d, NY))
    for peer in ring_y:
        signal(barrier, peer, gy)
    for other in across[:-1]:
        signal(barrier, chip_y * 16 + other, gy)
    for px in (up, down):
        for py in (left, right):
            signal(barrier, px, py)

    for load in loads[2:]:
        load.start()
    loads[0].wait()
    loads[1].wait()

    eight = lax.broadcasted_iota(jnp.int32, (8, 256), 0)
    z_lane = lax.broadcasted_iota(jnp.int32, (128, GZ), 1)

    def atoms_of(ref, x, s):
        return jnp.concatenate([ref[2 * x, s : s + 1, :], ref[2 * x + 1, s : s + 1, :]], axis=1)

    def deposit(x, carry):
        planes = jnp.concatenate([cell_ref[2 * x], cell_ref[2 * x + 1]], axis=0) // 128
        planes = jnp.transpose(planes)
        for s in range(8):
            cells = atoms_of(cell_ref, x, s)
            charge = atoms_of(chg_ref, x, s)
            hot = jnp.concatenate(
                [
                    jnp.where(z_lane == planes[:, 8 * r + s : 8 * r + s + 1], 1.0, 0.0).astype(BF16)
                    for r in range(2)
                ],
                axis=0,
            )
            high = charge.astype(BF16).astype(F32)
            rows = jnp.where(eight < 4, high, charge - high)
            rows = jnp.where(eight % 4 == cells % 4, rows, 0.0).astype(BF16)
            part = mxu(rows, hot)
            grid_t[x, s] = part[0:4] + part[4:8]
        return carry

    lax.fori_loop(0, 4, deposit, 0, unroll=True)

    tables[0].wait()
    ztrans = right_table(grid_t[...].reshape(128, GZ), casz)
    quarter = lane_block((32, 128))
    for h in range(2):
        parts = [ztrans[32 * x : 32 * x + 32, 128 * h : 128 * h + 128] for x in range(4)]
        for m in range(4):
            send_a[4 * h + m] = pick([turn(parts[x], x - m) for x in range(4)], quarter)

    pl.semaphore_wait(barrier, 7 + 7 + 15 + 4)

    def row_exchange(src, dst, which):
        for d in (4, 3, 5, 2, 6, 1, 7):
            peer = lax.rem(gy + d, NY)
            pltpu.make_async_remote_copy(
                src.at[peer],
                dst.at[gy],
                ex_send.at[which],
                ex_recv.at[which],
                device_id={"gx": gx, "gy": peer},
                device_id_type=MESH_ID,
            ).start()
        dst[gy] = src[gy]

    def row_wait(src, dst, which):
        pltpu.make_async_remote_copy(
            src.at[pl.ds(0, NY - 1)],
            dst.at[pl.ds(0, NY - 1)],
            ex_send.at[which],
            ex_recv.at[which],
            device_id={"gx": gx, "gy": right},
            device_id_type=MESH_ID,
        ).wait()

    def column_exchange(src, dst, which):
        each_column_peer(
            lambda peer: pltpu.make_async_remote_copy(
                src.at[peer],
                dst.at[gx],
                ex_send.at[which],
                ex_recv.at[which],
                device_id={"gx": peer, "gy": gy},
                device_id_type=MESH_ID,
            ).start()
        )
        dst[gx] = src[gx]

    def column_wait(src, dst, which):
        pltpu.make_async_remote_copy(
            src.at[pl.ds(0, NX - 1)],
            dst.at[pl.ds(0, NX - 1)],
            ex_send.at[which],
            ex_recv.at[which],
            device_id={"gx": up, "gy": gy},
            device_id_type=MESH_ID,
        ).wait()

    row_exchange(send_a, recv_a, 0)
    for peer in ring_y:
        signal(line_sem, peer, gy)

    kx = lax.broadcasted_iota(jnp.int32, (GX, 128), 0)
    lane = lax.broadcasted_iota(jnp.int32, (GX, 128), 1)
    kz = gy * 32 + lane % 32
    ky = gx * 2 + (lane // 32) % 2

    def wave(freq, length):
        part = jnp.minimum(freq, length - freq).astype(F32) * (1.0 / length)
        return part * part

    wave_sq = wave(kz, GZ) + wave(kx, GX) + wave(ky, GY)
    influence[...] = jnp.where(
        wave_sq > 0, 1.0 / (64.0 * jnp.where(wave_sq > 0, wave_sq, 1.0)), 0.0
    )

    tables[1].wait()
    row_wait(send_a, recv_a, 0)
    ytrans = left_table(casy, recv_a[...].reshape(GY, 128))
    send_b[...] = ytrans.reshape(NX, 2, 128)
    pl.semaphore_wait(line_sem, 7)
    column_exchange(send_b, recv_b, 1)

    loads[6].wait()
    for r in range(8):
        for c in range(3):
            halo[r + 1, 1:9, c, :] = pos_ref[c, r]
        halo[r + 1, 1:9, 3, :] = chg_ref[r]

    halo_copies = []
    for n, (dx, dy) in enumerate(
        ((-1, -1), (-1, 0), (-1, 1), (0, -1), (0, 1), (1, -1), (1, 0), (1, 1))
    ):
        px = (down, gx, up)[dx + 1]
        py = (left, gy, right)[dy + 1]
        src_r = {-1: pl.ds(1, 1), 0: pl.ds(1, 8), 1: pl.ds(8, 1)}[dx]
        dst_r = {-1: pl.ds(9, 1), 0: pl.ds(1, 8), 1: pl.ds(0, 1)}[dx]
        src_c = {-1: pl.ds(1, 1), 0: pl.ds(1, 8), 1: pl.ds(8, 1)}[dy]
        dst_c = {-1: pl.ds(9, 1), 0: pl.ds(1, 8), 1: pl.ds(0, 1)}[dy]
        copy = pltpu.make_async_remote_copy(
            halo.at[src_r, src_c],
            halo.at[dst_r, dst_c],
            halo_send.at[n],
            halo_recv.at[n],
            device_id={"gx": px, "gy": py},
            device_id_type=MESH_ID,
        )
        copy.start()
        halo_copies.append(copy)

    tables[2].wait()
    tables[3].wait()
    column_wait(send_b, recv_b, 1)
    lanes = lane_block((NX, 128))
    low_half = lax.broadcasted_iota(jnp.int32, (NX, 128), 1) < 64
    lines = [recv_b[:, e, :] for e in range(2)]
    turned = [[turn(lines[e], d) for d in range(4)] for e in range(2)]
    packed = []
    for x in range(4):
        value = pick([turned[b % 2][(b - x) % 4] for b in range(4)], lanes)
        high = value.astype(BF16).astype(F32)
        packed.append(jnp.where(low_half, high, value - high).astype(BF16))
    packed = jnp.concatenate(packed, axis=0)
    scaled = x_transform(casx, packed) * influence[...]
    high = scaled.astype(BF16).astype(F32)
    half = lax.broadcasted_iota(jnp.int32, (GX, 128), 1) < 64
    packed = jnp.where(half, high, scaled - high).astype(BF16)
    xback = x_transform(casxt, packed)
    plain = [xback[128 * x : 128 * x + 128] for x in range(4)]
    moved = [turn(p, 1) for p in plain]
    send_c[:, 0, :] = pick([plain[0], moved[1], plain[2], moved[3]], lanes)
    send_c[:, 1, :] = pick([moved[0], plain[1], moved[2], plain[3]], lanes)
    column_exchange(send_c, recv_c, 2)

    for copy in task_loads + halo_copies:
        copy.wait()

    def task_group(g, carry):
        firsts = []
        for t in range(8):
            patch = patch_s[0, 0, 8 * g + t]
            near = near_s[0, 0, 8 * g + t]
            prow, pcol = patch // 8 + 1, patch % 8 + 1
            drow, dcol = near // 3 - 1, near % 3 - 1
            firsts.append((prow, pcol, drow, dcol))
            second[4 * t : 4 * t + 4, :] = halo[prow + drow, pcol + dcol]
        columns = jnp.transpose(second[...])
        for t in range(8):
            prow, pcol, drow, dcol = firsts[t]
            first = halo[prow, pcol]
            ax = first[0:1] - drow.astype(F32) * PATCH_SIDE
            ay = first[1:2] - dcol.astype(F32) * PATCH_SIDE
            az = first[2:3]
            sums = [jnp.zeros((8, 128), F32) for _ in range(3)]
            for chunk in range(4):
                b = columns[32 * chunk : 32 * chunk + 32]
                delta = [
                    a - b[:, 4 * t + c : 4 * t + c + 1] for c, a in enumerate((ax, ay, az))
                ]
                dist = delta[0] * delta[0] + delta[1] * delta[1] + delta[2] * delta[2]
                inv = lax.rsqrt(dist + 1.0)
                weight = b[:, 4 * t + 3 : 4 * t + 4] * jnp.exp(dist * EXP_SCALE) * (inv * inv * inv)
                for c in range(3):
                    term = weight * delta[c]
                    sums[c] = sums[c] + (
                        (term[0:8] + term[8:16]) + (term[16:24] + term[24:32])
                    )
            for c in range(3):
                total = jnp.sum(sums[c], axis=0, keepdims=True) * first[3:4]
                task_force[c, pl.ds(8 * g + t, 1), :] = total
        return carry

    lax.fori_loop(0, TASKS // 8, task_group, 0)
    slot = lax.broadcasted_iota(jnp.int32, (64, TASKS), 1)
    owner = lax.broadcasted_iota(jnp.int32, (64, TASKS), 0)
    acts = jnp.where((owner == patch_ref[0]) & (slot < count_ref[...]), 1.0, 0.0).astype(BF16)
    for c in range(3):
        force = task_force[c]
        high = force.astype(BF16)
        rest = force - high.astype(F32)
        mid = rest.astype(BF16)
        low = (rest - mid.astype(F32)).astype(BF16)
        total = mxu(acts, high) + (mxu(acts, mid) + mxu(acts, low))
        forces_ref[c] = total.reshape(8, 8, 128)

    column_wait(send_c, recv_c, 2)
    yback = left_table(casy, recv_c[...].reshape(GY, 128))
    send_d[...] = yback.reshape(NY, 32, 128)
    row_exchange(send_d, recv_d, 3)
    row_wait(send_d, recv_d, 3)

    rows = []
    for x in range(4):
        halves = []
        for h in range(2):
            halves.append(
                pick([turn(recv_d[4 * h + m], m - x) for m in range(4)], quarter)
            )
        rows.append(jnp.concatenate(halves, axis=1))
    field = right_table(jnp.concatenate(rows, axis=0), casz) * (1.0 / (GX * GY * GZ))
    for h in range(2):
        half_z = field[:, 128 * h : 128 * h + 128].reshape(32, 4, 128)
        sampled[:, 4 * h : 4 * h + 4, :] = half_z

    row_code = lax.broadcasted_iota(jnp.int32, (8, 128), 0)
    for r in range(8):
        for s in range(8):
            cells = jnp.broadcast_to(cell_ref[r, s : s + 1, :], (8, 128))
            planes = cells // 128
            got = jnp.take_along_axis(sampled[(r // 2) * 8 + s], planes % 128, axis=1)
            code = (planes // 128) * 4 + cells % 4
            recip_ref[r, s : s + 1, :] = jnp.sum(
                jnp.where(row_code == code, got, 0.0), axis=0, keepdims=True
            )


def in_hbm(array):
    return pltpu.with_memory_space_constraint(array, pltpu.HBM)


def body(positions, charges, cell_index, task_patch, task_near, task_count):
    casz = cas_split(GZ)
    casy = cas_split(GY)
    order = (4 * np.arange(NX)[None, :] + np.arange(4)[:, None]).reshape(-1)
    casx = cas_split(GX, order)
    casxt = np.ascontiguousarray(np.swapaxes(casx, 1, 2))
    hbm = pl.BlockSpec(memory_space=pltpu.HBM)
    return pl.pallas_call(
        kernel,
        out_shape=(
            pltpu.VMEM((3, 8, 8, 128), F32),
            pltpu.VMEM((8, 8, 128), F32),
        ),
        in_specs=[hbm] * 10,
        out_specs=(pl.BlockSpec(memory_space=pltpu.VMEM),) * 2,
        scratch_shapes=[
            pltpu.SMEM((1, 1, TASKS), jnp.int32),
            pltpu.SMEM((1, 1, TASKS), jnp.int32),
            pltpu.VMEM((1, 1, TASKS), jnp.int32),
            pltpu.VMEM((1, 1), jnp.int32),
            pltpu.VMEM((3, 8, 8, 128), F32),
            pltpu.VMEM((8, 8, 128), F32),
            pltpu.VMEM((8, 8, 128), jnp.int32),
            pltpu.VMEM((2, GZ, GZ), BF16),
            pltpu.VMEM((2, GY, GY), BF16),
            pltpu.VMEM((2, GX, GX), BF16),
            pltpu.VMEM((2, GX, GX), BF16),
            pltpu.VMEM((10, 10, 4, 128), F32),
            pltpu.VMEM((4, 8, 4, GZ), F32),
            pltpu.VMEM((32, 8, 128), F32),
            pltpu.VMEM((GX, 128), F32),
            pltpu.VMEM((32, 128), F32),
            pltpu.VMEM((3, TASKS, 128), F32),
            pltpu.VMEM((NY, 32, 128), F32),
            pltpu.VMEM((NY, 32, 128), F32),
            pltpu.VMEM((NX, 2, 128), F32),
            pltpu.VMEM((NX, 2, 128), F32),
            pltpu.VMEM((NX, 2, 128), F32),
            pltpu.VMEM((NX, 2, 128), F32),
            pltpu.VMEM((NY, 32, 128), F32),
            pltpu.VMEM((NY, 32, 128), F32),
            pltpu.SemaphoreType.DMA((11,)),
            pltpu.SemaphoreType.DMA((8,)),
            pltpu.SemaphoreType.DMA((8,)),
            pltpu.SemaphoreType.DMA((4,)),
            pltpu.SemaphoreType.DMA((4,)),
            pltpu.SemaphoreType.REGULAR,
        ],
        compiler_params=pltpu.CompilerParams(
            collective_id=0, has_side_effects=True, vmem_limit_bytes=60 * 1024 * 1024
        ),
        name="patch_forces_and_grid",
    )(
        in_hbm(task_patch),
        in_hbm(task_near),
        task_count,
        in_hbm(positions),
        in_hbm(charges),
        in_hbm(cell_index),
        in_hbm(jnp.asarray(casz)),
        in_hbm(jnp.asarray(casy)),
        in_hbm(jnp.asarray(casx)),
        in_hbm(jnp.asarray(casxt)),
    )


def solution(mesh):
    return jax.shard_map(
        body,
        mesh=mesh,
        in_specs=(
            P(None, "gx", "gy", None),
            P("gx", "gy", None),
            P("gx", "gy", None),
            P("gx", "gy", None),
            P("gx", "gy", None),
            P("gx", "gy"),
        ),
        out_specs=(P(None, "gx", "gy", None), P("gx", "gy", None)),
        check_vma=False,
    )
```
